256 devices in a mesh: grp: 16 (over z, core), sub: 16 (over x, y).
Axes of the slice: x: 4, y: 4, z: 8, core: 2. Of those that a mesh axis runs over, the one named last changes fastest.
Arguments:
- coarse_op: float32 [256, 64, 576], P(('grp', 'sub'))
- right_side: float32 [256, 64, 64], P(('grp', 'sub')), may hold values from -6 to 6
- owner_map: int32 [256], replicated, may hold values from 0 to 255, as said below
- neighbor_table: int32 [256, 8], replicated, may hold values from 0 to 255, as said below
Outputs:
- solution: float32 [256, 64, 64], P(('grp', 'sub'))
The draws below stay inside these ranges and needn't reach their ends.
Inputs may be any that keep to these rules, and one draw needn't show every extreme that they name: `owner_map`: a permutation of 0 .. 255. `neighbor_table`: row t lists the neighbours of coarse site t on a periodic 4^4 lattice in the order +x, -x, +y, -y, +z, -z, +t, -t; lattice positions carry the site numbers in a permuted order.
All inputs are finite; a program needn't handle non-finite values.
Results may differ from the reference program's by a relative error of at most 0.0001.
Values sent between devices are 32-bit elements; how exact they have to be, the bound alone decides.
A program may use at most 64 MiB of HBM per device.

```python
import jax
import jax.numpy as jnp
from jax import lax

LAT = 4
DOF = 64
RHS = 64
ITERS = 3
HOPS = 8
SITES = 256


def draw_coarse_op(key, part):
    noise_key = jax.random.fold_in(key, 11)
    diag_key = jax.random.fold_in(key, 12)
    spread = 0.6 / (9.0 * DOF) ** 0.5
    noise = jax.random.normal(noise_key, (SITES, DOF, 9 * DOF), jnp.float32) * spread
    diag = jnp.exp(jax.random.uniform(diag_key, (SITES, DOF), jnp.float32, 0.0, 1.0986123))
    unit = jnp.eye(DOF, 9 * DOF, dtype=jnp.float32)
    return noise + diag[:, :, None] * unit[None]


def draw_owner_map(key, part):
    return jax.random.permutation(jax.random.fold_in(key, 21), SITES).astype(jnp.int32)


def draw_neighbor_table(key, part):
    relabel = jax.random.permutation(jax.random.fold_in(key, 31), SITES).astype(jnp.int32)
    position = jnp.arange(SITES, dtype=jnp.int32)
    columns = []
    for axis_dim in range(4):
        stride = LAT ** axis_dim
        coord = position // stride % LAT
        for offset in (1, -1):
            moved = position + ((coord + offset) % LAT - coord) * stride
            columns.append(relabel[moved])
    table = jnp.stack(columns, axis=1).astype(jnp.int32)
    return jnp.zeros((SITES, HOPS), jnp.int32).at[relabel].set(table)


def shard_levels(rng, dims, split, smallest, high):
    level, own = 1.0, jax.random.fold_in(rng, 6)
    for dim, shards_of in split:
        heights = jnp.exp(jax.random.uniform(jax.random.fold_in(own, dim), (shards_of,), jnp.float32, smallest / len(split), high / len(split)))
        level = level * jnp.repeat(heights, dims[dim] // shards_of).reshape([-1 if axis == dim else 1 for axis in range(len(dims))])
    return level


def gaussian(stream_key, dims, scale, limit, shards=(), held_as=jnp.bfloat16):
    array = scale * jax.random.normal(stream_key, dims, jnp.float32)
    if shards:
        array = array * shard_levels(stream_key, dims, shards, -0.22, 0.18)
    return jnp.clip(array, -limit, limit).astype(held_as)


def setup_inputs(seed: int = 0) -> dict:
    key_of = jax.random.split(jax.random.key(seed), 5)
    return {
        "coarse_op": draw_coarse_op(jax.random.fold_in(key_of[4], 71), 0),
        "right_side": gaussian(key_of[1], (SITES, DOF, RHS), 1.0, 6.0, ((0, 256),), jnp.float32),
        "owner_map": draw_owner_map(jax.random.fold_in(key_of[4], 71), 0),
        "neighbor_table": draw_neighbor_table(jax.random.fold_in(key_of[4], 71), 0),
    }


def inner_product(first, second):
    return lax.optimization_barrier(jnp.sum(first * second, axis=(0, 1)))

def reference(coarse_op, right_side, owner_map, neighbor_table):
    site_ids = jnp.arange(SITES, dtype=jnp.int32)
    inverse = lax.optimization_barrier(jnp.sum(jnp.where(owner_map[None, :] == site_ids[:, None], site_ids[None, :], 0), axis=1)).astype(jnp.int32)
    link = inverse[neighbor_table[owner_map]]

    def apply_op(vector):
        stacked = jnp.concatenate([vector[:, None], vector[link]], axis=1).reshape(SITES, 9 * DOF, RHS)
        return jnp.einsum('sac,scr->sar', coarse_op, stacked, precision=lax.Precision.HIGHEST)
    beta = jnp.sqrt(inner_product(right_side, right_side))
    krylov = [right_side / beta]
    hess = jnp.zeros((ITERS + 1, ITERS, RHS), jnp.float32)
    for column in range(ITERS):
        image = apply_op(krylov[column])
        coeffs = [inner_product(vector, image) for vector in krylov]
        for index_i in range(column + 1):
            image = image - coeffs[index_i] * krylov[index_i]
            hess = hess.at[index_i, column].set(coeffs[index_i])
        norm_value = jnp.sqrt(inner_product(image, image))
        hess = hess.at[column + 1, column].set(norm_value)
        krylov.append(image / norm_value)
    gram_matrix = jnp.einsum('ijr,ikr->rjk', hess, hess, precision=lax.Precision.HIGHEST)
    projected = (beta[None, :] * hess[0]).T
    weights = jnp.linalg.solve(gram_matrix, projected[..., None])[..., 0]
    solution = jnp.zeros_like(right_side)
    for column in range(ITERS):
        solution = solution + weights[:, column][None, None, :] * krylov[column]
    return solution
```

```python
import jax
import jax.numpy as jnp
from jax import lax
from jax.experimental import pallas as pl
from jax.experimental.pallas import tpu as pltpu
from jax.sharding import PartitionSpec as P

MESH = pl.DeviceIdType.MESH
NZ, NX, NY = 8, 4, 4
CH = 4
F32, BF16, I32 = jnp.float32, jnp.bfloat16, jnp.int32


def split(value):
    high = value.astype(BF16)
    return high, (value - high.astype(F32)).astype(BF16)


def dot_nt(left, right):
    return lax.dot_general(left, right, (((1,), (1,)), ((), ())), preferred_element_type=F32)


def fold8(value):
    return value.reshape(value.shape[0] // 8, 8, value.shape[1]).sum(axis=0)


def kernel(
    op_hbm, b_ref, om_ref, nt_ref, out_ref,
    opv, opb, wh, wl, pb, bb, z0, z1, z2, w1, w2, dh, dl, hot, xp, acc, pd, sb, ob,
    rx, tx_up, tx_dn, tx_sib, ld_sem, b_tx, b_rx, z_tx, z_rx, s_tx, s_rx,
):
    grp, sub = lax.axis_index("grp"), lax.axis_index("sub")
    z, core = grp // 2, grp % 2
    x, y = sub // NY, sub % NY

    def in_grp(e, q):
        return (z + e) % NZ * 2 + (core + q) % 2

    peers_z = [(e, q) for e in range(NZ) for q in range(2) if (e, q) != (0, 0)]
    peers_p = [(dx, dy) for dx in range(NX) for dy in range(NY) if (dx, dy) != (0, 0)]

    def plane(dx, dy):
        return {"grp": grp, "sub": (x + dx) % NX * NY + (y + dy) % NY}

    load = pltpu.make_async_copy(op_hbm.at[0], opv, ld_sem)
    load.start()
    barrier = pltpu.get_barrier_semaphore()
    for e, q in peers_z:
        pl.semaphore_signal(barrier, inc=1, device_id={"grp": in_grp(e, q), "sub": sub}, device_id_type=MESH)
    for dx, dy in peers_p:
        pl.semaphore_signal(barrier, inc=1, device_id=plane(dx, dy), device_id_type=MESH)

    bt = b_ref[0].T
    for p in range(2):
        pb[:, p, :] = jnp.concatenate([bt[32 * p : 32 * p + 16], bt[32 * p + 16 : 32 * p + 32]], axis=1)
    load.wait()
    for c in range(CH):
        for m in range(4):
            opb[0, 0, c, 16 * m : 16 * m + 16, :] = opv[16 * c : 16 * c + 16, 128 * m : 128 * m + 128]
        opb[0, 0, c, 64:72, :] = jnp.concatenate(
            [opv[16 * c : 16 * c + 8, 512:576], opv[16 * c + 8 : 16 * c + 16, 512:576]], axis=1
        )
    pl.semaphore_wait(barrier, len(peers_z) + len(peers_p))

    def op_copy(src, dst, send, grp_to):
        copy = pltpu.make_async_remote_copy(
            src_ref=opb.at[src], dst_ref=opb.at[dst], send_sem=send, recv_sem=rx.at[dst],
            device_id={"grp": grp_to, "sub": sub}, device_id_type=MESH,
        )
        copy.start()
        sends.append(copy)

    sends = []

    def go_up(e, c):
        op_copy((e, 0, c), ((e - 1) % NZ, 0, c), tx_up.at[(-e) % NZ, c], in_grp(1, 0))

    def go_down(e, c):
        op_copy((e, 0, c), (e + 1, 0, c), tx_dn.at[e, c], in_grp(NZ - 1, 0))

    def go_sib(e, c):
        op_copy((e, 0, c), (e, 1, c), tx_sib.at[e, c], in_grp(0, 1))

    def got(e, q, c):
        pltpu.make_async_copy(opb.at[e, q, c], opb.at[e, q, c], rx.at[e, q, c]).wait()

    for c in range(CH):
        go_up(0, c)
        go_down(0, c)
        go_sib(0, c)
    for e, q in peers_z:
        pltpu.make_async_remote_copy(
            src_ref=pb.at[in_grp(e, q)], dst_ref=bb.at[(NZ - e) % NZ * 2 + q], send_sem=b_tx, recv_sem=b_rx,
            device_id={"grp": in_grp(e, q), "sub": sub}, device_id_type=MESH,
        ).start()
    bb[0] = pb[grp]

    lane = lax.broadcasted_iota(I32, (16, 256), 1)
    row = lax.broadcasted_iota(I32, (16, 256), 0)
    own_slot = (((((row >> 1) + z) & 7) << 1) | (((row & 1) + core) & 1)) * 16 + sub
    om = jnp.broadcast_to(om_ref[...].astype(F32), (16, 256))
    lane_f = lane.astype(F32)
    own_site = jnp.sum(jnp.where(lane == own_slot, om, 0.0), axis=1, keepdims=True)
    pick = jnp.where(lane_f == own_site, 1.0, 0.0).astype(BF16)
    near = jnp.dot(pick, nt_ref[...].astype(F32).astype(BF16), preferred_element_type=F32)
    for k in range(8):
        slot = jnp.sum(jnp.where(om == near[:, k : k + 1], lane_f, 0.0), axis=1, keepdims=True).astype(I32)
        g_to, s_to = slot >> 4, slot & 15
        rel = ((((g_to >> 1) - z) & 7) << 1) | (((g_to & 1) - core) & 1)
        rel_s = ((((s_to >> 2) - x) & 3) << 2) | (((s_to & 3) - y) & 3)
        hot[16 * k : 16 * k + 16, :] = jnp.where(lane == rel_s * 16 + rel, 1.0, 0.0).astype(BF16)

    def convert(e, q):
        g, at = e // 2, (e % 2) * 128 + q * 64
        for c in range(CH):
            rows = slice(at + 16 * c, at + 16 * c + 16)
            for m in range(5):
                if m < 4:
                    piece = opb[e, q, c, 16 * m : 16 * m + 16, :]
                else:
                    tail = opb[e, q, c, 64:72, :]
                    piece = jnp.concatenate([tail, pltpu.roll(tail, 64, 1)], axis=0)
                high, low = split(piece)
                wh[g, rows, 128 * m : 128 * m + 128] = high
                wl[g, rows, 128 * m : 128 * m + 128] = low

    def take(e, q):
        if q == 1:
            for c in range(CH):
                got(e, 1, c)
        convert(e, q)

    def relay(step):
        for c in range(CH):
            e = NZ - step
            got(e, 0, c)
            if step < 3 or c < CH // 2:
                go_up(e, c)
            go_sib(e, c)
            e = step
            got(e, 0, c)
            if step < 3 or c >= CH // 2:
                go_down(e, c)
            go_sib(e, c)

    def spread(buf, n):
        for dx, dy in peers_p:
            pltpu.make_async_remote_copy(
                src_ref=buf.at[pl.ds(0, 16)], dst_ref=buf.at[pl.ds(((-dx) % NX * NY + (-dy) % NY) * 16, 16)],
                send_sem=z_tx.at[n], recv_sem=z_rx.at[n], device_id=plane(dx, dy), device_id_type=MESH,
            ).start()

    def arrived(buf, n):
        pltpu.make_async_copy(buf.at[pl.ds(16, 240)], buf.at[pl.ds(16, 240)], z_rx.at[n]).wait()

    left128 = lax.broadcasted_iota(I32, (16, 128), 1) < 64

    def segments(value):
        left = lax.broadcasted_iota(I32, (value.shape[0], 128), 1) < 64
        parts = []
        for t in range(value.shape[1] // 128):
            tile = value[:, 128 * t : 128 * t + 128]
            low = jnp.sum(jnp.where(left, tile, 0.0), axis=1, keepdims=True)
            high = jnp.sum(jnp.where(left, 0.0, tile), axis=1, keepdims=True)
            parts.append(jnp.where(left, low, high))
        return parts[0] if len(parts) == 1 else jnp.concatenate(parts, axis=1)

    def total(sums):
        return [segments(jnp.sum(part, axis=0, keepdims=True)) for part in sums]

    def build_x():
        near_h = jnp.dot(hot[...], dh[...], preferred_element_type=F32)
        near_l = jnp.dot(hot[...], dl[...], preferred_element_type=F32)
        for hl, (own, near_v) in enumerate(((dh, near_h), (dl, near_l))):
            for p in range(2):
                cols = slice(128 * p, 128 * p + 128)
                nat = [own[0:16, cols].astype(F32)] + [near_v[16 * k : 16 * k + 16, cols] for k in range(8)]
                rot = [pltpu.roll(part, 64, 1) for part in nat]
                for h in range(2):
                    first, second = (nat, rot) if h == 0 else (rot, nat)
                    at = (hl * 4 + p * 2 + h) * 16
                    for m in range(5):
                        right = second[2 * m + 1] if m < 4 else jnp.zeros((16, 128), F32)
                        xp[at : at + 16, 128 * m : 128 * m + 128] = jnp.where(left128, first[2 * m], right).astype(BF16)

    def apply_group(g, first):
        one = dot_nt(xp[...], wh[g])
        two = dot_nt(xp[0:64, :], wl[g])
        both = one[0:64] + one[64:128] + two
        r = lax.broadcasted_iota(I32, (64, 256), 0) & 15
        c = lax.broadcasted_iota(I32, (64, 256), 1) >> 6
        both = jnp.where(r == c + 4 * g, both, 0.0)
        acc[...] = both if first else acc[...] + both

    def image():
        half = acc[:, 0:128] + acc[:, 128:256]
        half = half + pltpu.roll(half, 64, 1)
        return jnp.concatenate([jnp.where(left128, half[32 * p : 32 * p + 16], half[32 * p + 16 : 32 * p + 32]) for p in range(2)], axis=1)

    rows_of = [slice(32 * i, 32 * i + 32) for i in range(8)]

    take(0, 0)
    take(0, 1)
    relay(1)
    pltpu.make_async_copy(bb.at[pl.ds(1, 15)], bb.at[pl.ds(1, 15)], b_rx).wait()
    for p in range(2):
        z0[0:16, 128 * p : 128 * p + 128] = bb[:, p, :]
    spread(z0, 0)
    for e in (1, 7):
        take(e, 0)
        take(e, 1)
    relay(2)
    for e in (2, 6):
        take(e, 0)
        take(e, 1)
    arrived(z0, 0)
    sums = jnp.zeros((8, 256), F32)
    for rows in rows_of:
        part = z0[rows, :]
        dh[rows, :], dl[rows, :] = split(part)
        sums = sums + fold8(part * part)
    beta = jnp.sqrt(total([sums])[0])
    s0 = 1.0 / beta
    build_x()
    relay(3)
    for e in (3, 5):
        take(e, 0)
        take(e, 1)
    apply_group(0, True)
    apply_group(3, False)
    apply_group(1, False)
    for c in range(CH):
        got(4, 0, c)
        go_sib(4, c)
    take(4, 0)
    take(4, 1)
    apply_group(2, False)

    def apply_all():
        for g in range(4):
            apply_group(g, g == 0)
        return image()

    z1[0:16, :] = image() * s0
    spread(z1, 1)
    arrived(z1, 1)
    sums = jnp.zeros((8, 256), F32)
    for rows in rows_of:
        sums = sums + fold8(z0[rows, :] * z1[rows, :])
    h00 = total([sums])[0] * s0
    f0 = h00 * s0
    sums = jnp.zeros((8, 256), F32)
    for rows in rows_of:
        part = z1[rows, :] - f0 * z0[rows, :]
        w1[rows, :] = part
        dh[rows, :], dl[rows, :] = split(part)
        sums = sums + fold8(part * part)
    build_x()
    h10 = jnp.sqrt(total([sums])[0])
    s1 = 1.0 / h10

    z2[0:16, :] = apply_all() * s1
    spread(z2, 2)
    r0 = jnp.sqrt(h00 * h00 + h10 * h10)
    i0 = 1.0 / r0
    c0, n0 = h00 * i0, h10 * i0
    g0, g1 = c0 * beta, -n0 * beta
    arrived(z2, 2)
    sums0, sums1 = jnp.zeros((8, 256), F32), jnp.zeros((8, 256), F32)
    for rows in rows_of:
        part = z2[rows, :]
        sums0 = sums0 + fold8(z0[rows, :] * part)
        sums1 = sums1 + fold8(w1[rows, :] * part)
    h01, h11 = total([sums0, sums1])
    h01, h11 = h01 * s0, h11 * s1
    f0, f1 = h01 * s0, h11 * s1
    sums = jnp.zeros((8, 256), F32)
    for rows in rows_of:
        part = z2[rows, :] - f0 * z0[rows, :] - f1 * w1[rows, :]
        if rows.start == 0:
            w2[...] = part[0:16]
        dh[rows, :], dl[rows, :] = split(part)
        sums = sums + fold8(part * part)
    build_x()
    h21 = jnp.sqrt(total([sums])[0])
    s2 = 1.0 / h21

    last = apply_all() * s2
    basis = [z0[0:16, :] * s0, w1[0:16, :] * s1, w2[...] * s2]
    sums = [jnp.sum(fold8(part * last), axis=0, keepdims=True) for part in basis + [last]]
    pd[0] = jnp.concatenate([part[:, 128 * p : 128 * p + 128] for part in sums for p in range(2)], axis=0)
    for dx, dy in peers_p:
        pltpu.make_async_remote_copy(
            src_ref=pd.at[0], dst_ref=pd.at[(-dx) % NX * NY + (-dy) % NY],
            send_sem=z_tx.at[3], recv_sem=z_rx.at[3], device_id=plane(dx, dy), device_id_type=MESH,
        ).start()
    t0, t1 = c0 * h01 + n0 * h11, c0 * h11 - n0 * h01
    r1 = jnp.sqrt(t1 * t1 + h21 * h21)
    i1 = 1.0 / r1
    c1, n1 = t1 * i1, h21 * i1
    g1, g2 = c1 * g1, -n1 * g1
    pltpu.make_async_copy(pd.at[pl.ds(1, 15)], pd.at[pl.ds(1, 15)], z_rx.at[3]).wait()
    dots = segments(jnp.sum(pd[...], axis=0))
    h02, h12, h22, zz = [jnp.concatenate([dots[2 * i : 2 * i + 1], dots[2 * i + 1 : 2 * i + 2]], axis=1) for i in range(4)]
    norm_sq = jnp.maximum(zz - h02 * h02 - h12 * h12 - h22 * h22, 0.0)
    u0, u1 = c0 * h02 + n0 * h12, c0 * h12 - n0 * h02
    u1, u2 = c1 * u1 + n1 * h22, c1 * h22 - n1 * u1
    y2 = u2 * g2 / (u2 * u2 + norm_sq)
    y1 = (g1 - u1 * y2) * i1
    y0 = (g0 - t0 * y1 - u0 * y2) * i0
    result = y0 * basis[0] + y1 * basis[1] + y2 * basis[2]
    for p in range(2):
        sb[:, p, :] = result[:, 128 * p : 128 * p + 128]
    for e, q in peers_z:
        pltpu.make_async_remote_copy(
            src_ref=sb.at[2 * e + q], dst_ref=ob.at[grp], send_sem=s_tx, recv_sem=s_rx,
            device_id={"grp": in_grp(e, q), "sub": sub}, device_id_type=MESH,
        ).start()
    ob[grp] = sb[0]
    for copy in sends:
        copy.wait_send()
    pltpu.make_async_copy(pb.at[pl.ds(1, 15)], pb.at[pl.ds(1, 15)], b_tx).wait()
    for n, buf in enumerate((z0, z1, z2)):
        pltpu.make_async_copy(buf.at[pl.ds(16, 240)], buf.at[pl.ds(16, 240)], z_tx.at[n]).wait()
    pltpu.make_async_copy(pd.at[pl.ds(1, 15)], pd.at[pl.ds(1, 15)], z_tx.at[3]).wait()
    pltpu.make_async_copy(sb.at[pl.ds(1, 15)], sb.at[pl.ds(1, 15)], s_tx).wait()
    pltpu.make_async_copy(ob.at[pl.ds(1, 15)], ob.at[pl.ds(1, 15)], s_rx).wait()
    tiles = [ob[:, p, :] for p in range(2)]
    out_ref[0] = jnp.concatenate(
        [tiles[0][:, 0:64], tiles[0][:, 64:128], tiles[1][:, 0:64], tiles[1][:, 64:128]], axis=0
    ).T


def per_device(coarse_op, right_side, owner_map, neighbor_table):
    vmem = pl.BlockSpec(memory_space=pltpu.VMEM)
    dma = pltpu.SemaphoreType.DMA
    return pl.pallas_call(
        kernel,
        out_shape=jax.ShapeDtypeStruct((1, 64, 64), F32),
        in_specs=[pl.BlockSpec(memory_space=pl.ANY), vmem, vmem, vmem],
        out_specs=vmem,
        scratch_shapes=[
            pltpu.VMEM((64, 576), F32),
            pltpu.VMEM((NZ, 2, CH, 72, 128), F32),
            pltpu.VMEM((4, 256, 640), BF16),
            pltpu.VMEM((4, 256, 640), BF16),
            pltpu.VMEM((16, 2, 128), F32),
            pltpu.VMEM((16, 2, 128), F32),
            pltpu.VMEM((256, 256), F32),
            pltpu.VMEM((256, 256), F32),
            pltpu.VMEM((256, 256), F32),
            pltpu.VMEM((256, 256), F32),
            pltpu.VMEM((16, 256), F32),
            pltpu.VMEM((256, 256), BF16),
            pltpu.VMEM((256, 256), BF16),
            pltpu.VMEM((128, 256), BF16),
            pltpu.VMEM((128, 640), BF16),
            pltpu.VMEM((64, 256), F32),
            pltpu.VMEM((16, 8, 128), F32),
            pltpu.VMEM((16, 2, 128), F32),
            pltpu.VMEM((16, 2, 128), F32),
            dma((NZ, 2, CH)),
            dma((4, CH)),
            dma((4, CH)),
            dma((NZ, CH)),
            dma,
            dma,
            dma,
            dma((4,)),
            dma((4,)),
            dma,
            dma,
        ],
        compiler_params=pltpu.CompilerParams(collective_id=0, has_side_effects=True),
    )(coarse_op, right_side, owner_map.reshape(1, 256), neighbor_table)


def solution(mesh):
    placed = (P(("grp", "sub"), None, None), P(("grp", "sub"), None, None), P(), P())
    return jax.shard_map(
        per_device,
        mesh=mesh,
        in_specs=placed,
        out_specs=P(("grp", "sub"), None, None),
        check_vma=False,
    )
```

```python
import jax
import jax.numpy as jnp
from jax import lax
from jax.experimental import pallas as pl
from jax.experimental.pallas import tpu as pltpu
from jax.sharding import PartitionSpec as P

MESH = pl.DeviceIdType.MESH
NZ, NX, NY = 8, 4, 4
CH = 4
F32, BF16, I32 = jnp.float32, jnp.bfloat16, jnp.int32


def split(value):
    high = value.astype(BF16)
    return high, (value - high.astype(F32)).astype(BF16)


def dot_nt(left, right):
    return lax.dot_general(left, right, (((1,), (1,)), ((), ())), preferred_element_type=F32)


def fold8(value):
    return value.reshape(value.shape[0] // 8, 8, value.shape[1]).sum(axis=0)


def kernel(
    op_hbm, b_hbm, om_hbm, nt_hbm, out_ref,
    b_ref, om_ref, nt_ref, opv, opb, wh, wl, pb, bb, z0, z1, z2, w1, w2, dh, dl, hot, xp, acc, pd, sb, ob,
    rx, tx_up, tx_dn, tx_sib, ld_sem, b_tx, b_rx, z_tx, z_rx, s_tx, s_rx,
):
    grp, sub = lax.axis_index("grp"), lax.axis_index("sub")
    z, core = grp // 2, grp % 2
    x, y = sub // NY, sub % NY

    def in_grp(e, q):
        return (z + e) % NZ * 2 + (core + q) % 2

    def hops(*steps):
        return sum(min(step, size - step) for step, size in steps)

    peers_z = [(e, q) for e in range(NZ) for q in range(2) if (e, q) != (0, 0)]
    peers_p = [(dx, dy) for dx in range(NX) for dy in range(NY) if (dx, dy) != (0, 0)]
    peers_z.sort(key=lambda peer: -hops((peer[0], NZ)))
    peers_p.sort(key=lambda peer: -hops((peer[0], NX), (peer[1], NY)))

    def plane(dx, dy):
        return {"grp": grp, "sub": (x + dx) % NX * NY + (y + dy) % NY}

    barrier = pltpu.get_barrier_semaphore()
    for e, q in peers_z:
        pl.semaphore_signal(barrier, inc=1, device_id={"grp": in_grp(e, q), "sub": sub}, device_id_type=MESH)
    for dx, dy in peers_p:
        pl.semaphore_signal(barrier, inc=1, device_id=plane(dx, dy), device_id_type=MESH)

    ins = ((b_hbm.at[0], b_ref), (op_hbm.at[0], opv), (om_hbm, om_ref), (nt_hbm, nt_ref))
    loads = [pltpu.make_async_copy(src, dst, ld_sem.at[n]) for n, (src, dst) in enumerate(ins)]
    for load in loads:
        load.start()

    loads[0].wait()
    bt = b_ref[...].T
    for p in range(2):
        pb[:, p, :] = jnp.concatenate([bt[32 * p : 32 * p + 16], bt[32 * p + 16 : 32 * p + 32]], axis=1)
    loads[1].wait()
    for c in range(CH):
        for m in range(4):
            opb[0, 0, c, 16 * m : 16 * m + 16, :] = opv[16 * c : 16 * c + 16, 128 * m : 128 * m + 128]
        opb[0, 0, c, 64:72, :] = jnp.concatenate(
            [opv[16 * c : 16 * c + 8, 512:576], opv[16 * c + 8 : 16 * c + 16, 512:576]], axis=1
        )
    pl.semaphore_wait(barrier, len(peers_z) + len(peers_p))

    def op_copy(src, dst, send, grp_to):
        copy = pltpu.make_async_remote_copy(
            src_ref=opb.at[src], dst_ref=opb.at[dst], send_sem=send, recv_sem=rx.at[dst],
            device_id={"grp": grp_to, "sub": sub}, device_id_type=MESH,
        )
        copy.start()
        sends.append(copy)

    sends = []

    def go_up(e, c):
        op_copy((e, 0, c), ((e - 1) % NZ, 0, c), tx_up.at[(-e) % NZ, c], in_grp(1, 0))

    def go_down(e, c):
        op_copy((e, 0, c), (e + 1, 0, c), tx_dn.at[e, c], in_grp(NZ - 1, 0))

    def go_sib(e, c):
        op_copy((e, 0, c), (e, 1, c), tx_sib.at[e, c], in_grp(0, 1))

    def got(e, q, c):
        pltpu.make_async_copy(opb.at[e, q, c], opb.at[e, q, c], rx.at[e, q, c]).wait()

    for e, q in peers_z:
        pltpu.make_async_remote_copy(
            src_ref=pb.at[in_grp(e, q)], dst_ref=bb.at[(NZ - e) % NZ * 2 + q], send_sem=b_tx, recv_sem=b_rx,
            device_id={"grp": in_grp(e, q), "sub": sub}, device_id_type=MESH,
        ).start()
    for c in range(CH):
        go_up(0, c)
        go_down(0, c)
        go_sib(0, c)
    bb[0] = pb[grp]

    loads[2].wait()
    loads[3].wait()
    lane = lax.broadcasted_iota(I32, (16, 256), 1)
    row = lax.broadcasted_iota(I32, (16, 256), 0)
    own_slot = (((((row >> 1) + z) & 7) << 1) | (((row & 1) + core) & 1)) * 16 + sub
    om = jnp.broadcast_to(om_ref[...].astype(F32), (16, 256))
    lane_f = lane.astype(F32)
    own_site = jnp.sum(jnp.where(lane == own_slot, om, 0.0), axis=1, keepdims=True)
    pick = jnp.where(lane_f == own_site, 1.0, 0.0).astype(BF16)
    near = dot_nt(pick, nt_ref[...].astype(F32).astype(BF16))
    for k in range(8):
        slot = jnp.sum(jnp.where(om == near[:, k : k + 1], lane_f, 0.0), axis=1, keepdims=True).astype(I32)
        g_to, s_to = slot >> 4, slot & 15
        rel = ((((g_to >> 1) - z) & 7) << 1) | (((g_to & 1) - core) & 1)
        rel_s = ((((s_to >> 2) - x) & 3) << 2) | (((s_to & 3) - y) & 3)
        hot[16 * k : 16 * k + 16, :] = jnp.where(lane == rel_s * 16 + rel, 1.0, 0.0).astype(BF16)

    def take(e):
        for c in range(CH):
            got(e, 1, c)
        at = slice(e % 2 * 128, e % 2 * 128 + 128)
        for m in range(5):
            pieces = []
            for q in range(2):
                for c in range(CH):
                    if m < 4:
                        pieces.append(opb[e, q, c, 16 * m : 16 * m + 16, :])
                    else:
                        tail = opb[e, q, c, 64:72, :]
                        pieces += [tail, pltpu.roll(tail, 64, 1)]
            turned = jnp.concatenate(pieces, axis=0).T
            depth = 128 if m < 4 else 64
            high, low = split(turned[0:depth])
            wh[e // 2, 128 * m : 128 * m + depth, at] = high
            wl[e // 2, 128 * m : 128 * m + depth, at] = low

    def relay(step):
        for c in range(CH):
            e = NZ - step
            got(e, 0, c)
            if step < 3 or c < CH // 2:
                go_up(e, c)
            go_sib(e, c)
            e = step
            got(e, 0, c)
            if step < 3 or c >= CH // 2:
                go_down(e, c)
            go_sib(e, c)

    def spread(buf, n):
        for dx, dy in peers_p:
            pltpu.make_async_remote_copy(
                src_ref=buf.at[pl.ds(0, 16)], dst_ref=buf.at[pl.ds(((-dx) % NX * NY + (-dy) % NY) * 16, 16)],
                send_sem=z_tx.at[n], recv_sem=z_rx.at[n], device_id=plane(dx, dy), device_id_type=MESH,
            ).start()

    def arrived(buf, n):
        pltpu.make_async_copy(buf.at[pl.ds(16, 240)], buf.at[pl.ds(16, 240)], z_rx.at[n]).wait()

    left128 = lax.broadcasted_iota(I32, (16, 128), 1) < 64

    def segments(value):
        left = lax.broadcasted_iota(I32, (value.shape[0], 128), 1) < 64
        parts = []
        for t in range(value.shape[1] // 128):
            tile = value[:, 128 * t : 128 * t + 128]
            low = jnp.sum(jnp.where(left, tile, 0.0), axis=1, keepdims=True)
            high = jnp.sum(jnp.where(left, 0.0, tile), axis=1, keepdims=True)
            parts.append(jnp.where(left, low, high))
        return parts[0] if len(parts) == 1 else jnp.concatenate(parts, axis=1)

    def total(sums):
        return [segments(jnp.sum(part, axis=0, keepdims=True)) for part in sums]

    def build_x():
        near_h = jnp.dot(hot[...], dh[...], preferred_element_type=F32)
        near_l = jnp.dot(hot[...], dl[...], preferred_element_type=F32)
        for hl, (own, near_v) in enumerate(((dh, near_h), (dl, near_l))):
            for p in range(2):
                cols = slice(128 * p, 128 * p + 128)
                nat = [own[0:16, cols].astype(F32)] + [near_v[16 * k : 16 * k + 16, cols] for k in range(8)]
                rot = [pltpu.roll(part, 64, 1) for part in nat]
                for h in range(2):
                    first, second = (nat, rot) if h == 0 else (rot, nat)
                    at = (hl * 4 + p * 2 + h) * 16
                    for m in range(4):
                        both = jnp.where(left128, first[2 * m], second[2 * m + 1])
                        xp[at : at + 16, 128 * m : 128 * m + 128] = both.astype(BF16)
                    xp[at : at + 16, 512:576] = first[8][:, 0:64].astype(BF16)

    def apply_group(g, first):
        one = jnp.dot(xp[...], wh[g], preferred_element_type=F32)
        two = jnp.dot(xp[0:64, :], wl[g], preferred_element_type=F32)
        both = one[0:64] + one[64:128] + two
        r = lax.broadcasted_iota(I32, (64, 256), 0) & 15
        c = lax.broadcasted_iota(I32, (64, 256), 1) >> 6
        both = jnp.where(r == c + 4 * g, both, 0.0)
        acc[...] = both if first else acc[...] + both

    def image():
        half = acc[:, 0:128] + acc[:, 128:256]
        half = half + pltpu.roll(half, 64, 1)
        return jnp.concatenate([jnp.where(left128, half[32 * p : 32 * p + 16], half[32 * p + 16 : 32 * p + 32]) for p in range(2)], axis=1)

    rows_of = [slice(32 * i, 32 * i + 32) for i in range(8)]

    take(0)
    relay(1)
    pltpu.make_async_copy(bb.at[pl.ds(1, 15)], bb.at[pl.ds(1, 15)], b_rx).wait()
    for p in range(2):
        z0[0:16, 128 * p : 128 * p + 128] = bb[:, p, :]
    spread(z0, 0)
    for e in (1, 7):
        take(e)
    relay(2)
    for e in (2, 6):
        take(e)
    arrived(z0, 0)
    sums = jnp.zeros((8, 256), F32)
    for rows in rows_of:
        part = z0[rows, :]
        dh[rows, :], dl[rows, :] = split(part)
        sums = sums + fold8(part * part)
    beta = jnp.sqrt(total([sums])[0])
    s0 = 1.0 / beta
    build_x()
    relay(3)
    for e in (3, 5):
        take(e)
    apply_group(0, True)
    apply_group(3, False)
    apply_group(1, False)
    for c in range(CH):
        got(4, 0, c)
        go_sib(4, c)
    take(4)
    apply_group(2, False)

    def apply_all():
        for g in range(4):
            apply_group(g, g == 0)
        return image()

    z1[0:16, :] = image() * s0
    spread(z1, 1)
    arrived(z1, 1)
    sums = jnp.zeros((8, 256), F32)
    for rows in rows_of:
        sums = sums + fold8(z0[rows, :] * z1[rows, :])
    h00 = total([sums])[0] * s0
    f0 = h00 * s0
    sums = jnp.zeros((8, 256), F32)
    for rows in rows_of:
        part = z1[rows, :] - f0 * z0[rows, :]
        w1[rows, :] = part
        dh[rows, :], dl[rows, :] = split(part)
        sums = sums + fold8(part * part)
    build_x()
    h10 = jnp.sqrt(total([sums])[0])
    s1 = 1.0 / h10

    z2[0:16, :] = apply_all() * s1
    spread(z2, 2)
    r0 = jnp.sqrt(h00 * h00 + h10 * h10)
    i0 = 1.0 / r0
    c0, n0 = h00 * i0, h10 * i0
    g0, g1 = c0 * beta, -n0 * beta
    arrived(z2, 2)
    sums0, sums1 = jnp.zeros((8, 256), F32), jnp.zeros((8, 256), F32)
    for rows in rows_of:
        part = z2[rows, :]
        sums0 = sums0 + fold8(z0[rows, :] * part)
        sums1 = sums1 + fold8(w1[rows, :] * part)
    h01, h11 = total([sums0, sums1])
    h01, h11 = h01 * s0, h11 * s1
    f0, f1 = h01 * s0, h11 * s1
    sums = jnp.zeros((8, 256), F32)
    for rows in rows_of:
        part = z2[rows, :] - f0 * z0[rows, :] - f1 * w1[rows, :]
        if rows.start == 0:
            w2[...] = part[0:16]
        dh[rows, :], dl[rows, :] = split(part)
        sums = sums + fold8(part * part)
    build_x()
    h21 = jnp.sqrt(total([sums])[0])
    s2 = 1.0 / h21

    last = apply_all() * s2
    basis = [z0[0:16, :] * s0, w1[0:16, :] * s1, w2[...] * s2]
    sums = [jnp.sum(fold8(part * last), axis=0, keepdims=True) for part in basis + [last]]
    pd[0] = jnp.concatenate([part[:, 128 * p : 128 * p + 128] for part in sums for p in range(2)], axis=0)
    for dx, dy in peers_p:
        pltpu.make_async_remote_copy(
            src_ref=pd.at[0], dst_ref=pd.at[(-dx) % NX * NY + (-dy) % NY],
            send_sem=z_tx.at[3], recv_sem=z_rx.at[3], device_id=plane(dx, dy), device_id_type=MESH,
        ).start()
    t0, t1 = c0 * h01 + n0 * h11, c0 * h11 - n0 * h01
    r1 = jnp.sqrt(t1 * t1 + h21 * h21)
    i1 = 1.0 / r1
    c1, n1 = t1 * i1, h21 * i1
    g1, g2 = c1 * g1, -n1 * g1
    pltpu.make_async_copy(pd.at[pl.ds(1, 15)], pd.at[pl.ds(1, 15)], z_rx.at[3]).wait()
    dots = segments(jnp.sum(pd[...], axis=0))
    h02, h12, h22, zz = [jnp.concatenate([dots[2 * i : 2 * i + 1], dots[2 * i + 1 : 2 * i + 2]], axis=1) for i in range(4)]
    norm_sq = jnp.maximum(zz - h02 * h02 - h12 * h12 - h22 * h22, 0.0)
    u0, u1 = c0 * h02 + n0 * h12, c0 * h12 - n0 * h02
    u1, u2 = c1 * u1 + n1 * h22, c1 * h22 - n1 * u1
    y2 = u2 * g2 / (u2 * u2 + norm_sq)
    y1 = (g1 - u1 * y2) * i1
    y0 = (g0 - t0 * y1 - u0 * y2) * i0
    result = y0 * basis[0] + y1 * basis[1] + y2 * basis[2]
    for p in range(2):
        sb[:, p, :] = result[:, 128 * p : 128 * p + 128]
    for e, q in peers_z:
        pltpu.make_async_remote_copy(
            src_ref=sb.at[2 * e + q], dst_ref=ob.at[grp], send_sem=s_tx, recv_sem=s_rx,
            device_id={"grp": in_grp(e, q), "sub": sub}, device_id_type=MESH,
        ).start()
    ob[grp] = sb[0]
    for copy in sends:
        copy.wait_send()
    pltpu.make_async_copy(pb.at[pl.ds(1, 15)], pb.at[pl.ds(1, 15)], b_tx).wait()
    for n, buf in enumerate((z0, z1, z2)):
        pltpu.make_async_copy(buf.at[pl.ds(16, 240)], buf.at[pl.ds(16, 240)], z_tx.at[n]).wait()
    pltpu.make_async_copy(pd.at[pl.ds(1, 15)], pd.at[pl.ds(1, 15)], z_tx.at[3]).wait()
    pltpu.make_async_copy(sb.at[pl.ds(1, 15)], sb.at[pl.ds(1, 15)], s_tx).wait()
    pltpu.make_async_copy(ob.at[pl.ds(1, 15)], ob.at[pl.ds(1, 15)], s_rx).wait()
    tiles = [ob[:, p, :] for p in range(2)]
    out_ref[0] = jnp.concatenate(
        [tiles[0][:, 0:64], tiles[0][:, 64:128], tiles[1][:, 0:64], tiles[1][:, 64:128]], axis=0
    ).T


def per_device(coarse_op, right_side, owner_map, neighbor_table):
    vmem = pl.BlockSpec(memory_space=pltpu.VMEM)
    dma = pltpu.SemaphoreType.DMA
    return pl.pallas_call(
        kernel,
        out_shape=jax.ShapeDtypeStruct((1, 64, 64), F32),
        in_specs=[pl.BlockSpec(memory_space=pl.ANY)] * 4,
        out_specs=vmem,
        scratch_shapes=[
            pltpu.VMEM((64, 64), F32),
            pltpu.VMEM((1, 256), I32),
            pltpu.VMEM((8, 256), I32),
            pltpu.VMEM((64, 576), F32),
            pltpu.VMEM((NZ, 2, CH, 72, 128), F32),
            pltpu.VMEM((4, 576, 256), BF16),
            pltpu.VMEM((4, 576, 256), BF16),
            pltpu.VMEM((16, 2, 128), F32),
            pltpu.VMEM((16, 2, 128), F32),
            pltpu.VMEM((256, 256), F32),
            pltpu.VMEM((256, 256), F32),
            pltpu.VMEM((256, 256), F32),
            pltpu.VMEM((256, 256), F32),
            pltpu.VMEM((16, 256), F32),
            pltpu.VMEM((256, 256), BF16),
            pltpu.VMEM((256, 256), BF16),
            pltpu.VMEM((128, 256), BF16),
            pltpu.VMEM((128, 576), BF16),
            pltpu.VMEM((64, 256), F32),
            pltpu.VMEM((16, 8, 128), F32),
            pltpu.VMEM((16, 2, 128), F32),
            pltpu.VMEM((16, 2, 128), F32),
            dma((NZ, 2, CH)),
            dma((4, CH)),
            dma((4, CH)),
            dma((NZ, CH)),
            dma((4,)),
            dma,
            dma,
            dma((4,)),
            dma((4,)),
            dma,
            dma,
        ],
        compiler_params=pltpu.CompilerParams(collective_id=0, has_side_effects=True),
    )(coarse_op, right_side, owner_map.reshape(1, 256), neighbor_table.T)


def solution(mesh):
    placed = (P(("grp", "sub"), None, None), P(("grp", "sub"), None, None), P(), P())
    return jax.shard_map(
        per_device,
        mesh=mesh,
        in_specs=placed,
        out_specs=P(("grp", "sub"), None, None),
        check_vma=False,
    )
```

```python
import jax
import jax.numpy as jnp
from jax import lax
from jax.experimental import pallas as pl
from jax.experimental.pallas import tpu as pltpu
from jax.sharding import PartitionSpec as P

MESH = pl.DeviceIdType.MESH
NZ, NX, NY = 8, 4, 4
CH = 9
F32, BF16, I32 = jnp.float32, jnp.bfloat16, jnp.int32


def split(value):
    high = value.astype(BF16)
    return high, (value - high.astype(F32)).astype(BF16)


def dot_nt(left, right):
    return lax.dot_general(left, right, (((1,), (1,)), ((), ())), preferred_element_type=F32)


def fold8(value):
    return value.reshape(value.shape[0] // 8, 8, value.shape[1]).sum(axis=0)


def kernel(
    op_hbm, b_hbm, om_hbm, nt_hbm, out_ref,
    b_ref, om_ref, nt_ref, opv, opb, wh, wl, pb, bb, z0, z1, z2, w1, w2, dh, dl, hot, xp, acc, pd, sb, ob,
    rx, rx4, sib_rx, op_tx, ld_sem, b_tx, b_rx, z_tx, z_rx, s_tx, s_rx,
):
    grp, sub = lax.axis_index("grp"), lax.axis_index("sub")
    z, core = grp // 2, grp % 2
    x, y = sub // NY, sub % NY

    def in_grp(e, q):
        return (z + e) % NZ * 2 + (core + q) % 2

    def hops(*steps):
        return sum(min(step, size - step) for step, size in steps)

    peers_z = [(e, q) for e in range(NZ) for q in range(2) if (e, q) != (0, 0)]
    peers_p = [(dx, dy) for dx in range(NX) for dy in range(NY) if (dx, dy) != (0, 0)]
    peers_z.sort(key=lambda peer: -hops((peer[0], NZ)))
    peers_p.sort(key=lambda peer: -hops((peer[0], NX), (peer[1], NY)))

    def plane(dx, dy):
        return {"grp": grp, "sub": (x + dx) % NX * NY + (y + dy) % NY}

    barrier = pltpu.get_barrier_semaphore()
    for e, q in peers_z:
        pl.semaphore_signal(barrier, inc=1, device_id={"grp": in_grp(e, q), "sub": sub}, device_id_type=MESH)
    for dx, dy in peers_p:
        pl.semaphore_signal(barrier, inc=1, device_id=plane(dx, dy), device_id_type=MESH)

    ins = ((b_hbm.at[0], b_ref), (op_hbm.at[0], opv), (om_hbm, om_ref), (nt_hbm, nt_ref))
    loads = [pltpu.make_async_copy(src, dst, ld_sem.at[n]) for n, (src, dst) in enumerate(ins)]
    for load in loads:
        load.start()

    loads[0].wait()
    bt = b_ref[...].T
    for p in range(2):
        pb[:, p, :] = jnp.concatenate([bt[32 * p : 32 * p + 16], bt[32 * p + 16 : 32 * p + 32]], axis=1)
    loads[1].wait()
    for c in range(CH - 1):
        rows, m = c % 2 * 32, c // 2 * 128
        opb[0, 0, c] = opv[rows : rows + 32, m : m + 128]
    opb[0, 0, CH - 1] = jnp.concatenate([opv[0:32, 512:576], opv[32:64, 512:576]], axis=1)
    pl.semaphore_wait(barrier, len(peers_z) + len(peers_p))

    sent = []

    def op_copy(e, to, q, c, count, sem, grp_to):
        pltpu.make_async_remote_copy(
            src_ref=opb.at[e, 0, pl.ds(c, count)], dst_ref=opb.at[to, q, pl.ds(c, count)], send_sem=op_tx, recv_sem=sem,
            device_id={"grp": grp_to, "sub": sub}, device_id_type=MESH,
        ).start()
        sent.append(count)

    def ring(e, to, c, count, grp_to):
        if to == 4:
            for at in range(c, c + count):
                if (at < CH // 2) == (e == 5):
                    op_copy(e, to, 0, at, 1, rx4.at[at], grp_to)
        else:
            op_copy(e, to, 0, c, count, rx.at[to, c // 2], grp_to)

    def go_up(e, c, count):
        ring(e, (e - 1) % NZ, c, count, in_grp(1, 0))

    def go_down(e, c, count):
        ring(e, e + 1, c, count, in_grp(NZ - 1, 0))

    def go_sib(e, c, count):
        op_copy(e, e, 1, c, count, sib_rx.at[e], in_grp(0, 1))

    def got(ref, sem):
        pltpu.make_async_copy(ref, ref, sem).wait()

    pieces_of = [(c, min(2, CH - c)) for c in range(0, CH, 2)]

    for e, q in peers_z:
        pltpu.make_async_remote_copy(
            src_ref=pb.at[in_grp(e, q)], dst_ref=bb.at[(NZ - e) % NZ * 2 + q], send_sem=b_tx, recv_sem=b_rx,
            device_id={"grp": in_grp(e, q), "sub": sub}, device_id_type=MESH,
        ).start()
    for c, count in pieces_of:
        go_up(0, c, count)
        go_down(0, c, count)
        go_sib(0, c, count)
    bb[0] = pb[grp]

    loads[2].wait()
    loads[3].wait()
    lane = lax.broadcasted_iota(I32, (16, 256), 1)
    row = lax.broadcasted_iota(I32, (16, 256), 0)
    own_slot = (((((row >> 1) + z) & 7) << 1) | (((row & 1) + core) & 1)) * 16 + sub
    om = jnp.broadcast_to(om_ref[...].astype(F32), (16, 256))
    lane_f = lane.astype(F32)
    own_site = jnp.sum(jnp.where(lane == own_slot, om, 0.0), axis=1, keepdims=True)
    pick = jnp.where(lane_f == own_site, 1.0, 0.0).astype(BF16)
    near = dot_nt(pick, nt_ref[...].astype(F32).astype(BF16))
    for k in range(8):
        slot = jnp.sum(jnp.where(om == near[:, k : k + 1], lane_f, 0.0), axis=1, keepdims=True).astype(I32)
        g_to, s_to = slot >> 4, slot & 15
        rel = ((((g_to >> 1) - z) & 7) << 1) | (((g_to & 1) - core) & 1)
        rel_s = ((((s_to >> 2) - x) & 3) << 2) | (((s_to & 3) - y) & 3)
        hot[16 * k : 16 * k + 16, :] = jnp.where(lane == rel_s * 16 + rel, 1.0, 0.0).astype(BF16)

    def take(e):
        at = slice(e % 2 * 128, e % 2 * 128 + 128)
        got(opb.at[e, 1], sib_rx.at[e])
        for m in range(5):
            pieces = []
            for q in range(2):
                for c in range(2 * m, min(2 * m + 2, CH)):
                    pieces.append(opb[e, q, c])
                    if m == 4:
                        pieces.append(pltpu.roll(pieces[-1], 64, 1))
            turned = jnp.concatenate(pieces, axis=0).T
            depth = 128 if m < 4 else 64
            high, low = split(turned[0:depth])
            wh[e // 2, 128 * m : 128 * m + depth, at] = high
            wl[e // 2, 128 * m : 128 * m + depth, at] = low

    def relay(step):
        for c, count in pieces_of:
            for e, go in ((NZ - step, go_up), (step, go_down)):
                got(opb.at[e, 0, pl.ds(c, count)], rx.at[e, c // 2])
                go(e, c, count)
                go_sib(e, c, count)

    def last_block(*pieces):
        for c in pieces:
            got(opb.at[4, 0, c], rx4.at[c])
            go_sib(4, c, 1)

    def spread(buf, n, at=0, count=16):
        for dx, dy in peers_p:
            pltpu.make_async_remote_copy(
                src_ref=buf.at[pl.ds(at, count)],
                dst_ref=buf.at[pl.ds(((-dx) % NX * NY + (-dy) % NY) * 16 + at, count)],
                send_sem=z_tx.at[n], recv_sem=z_rx.at[n], device_id=plane(dx, dy), device_id_type=MESH,
            ).start()

    def arrived(buf, n):
        pltpu.make_async_copy(buf.at[pl.ds(16, 240)], buf.at[pl.ds(16, 240)], z_rx.at[n]).wait()

    left8 = lax.broadcasted_iota(I32, (8, 128), 1) < 64

    def segments(value):
        left = lax.broadcasted_iota(I32, (value.shape[0], 128), 1) < 64
        parts = []
        for t in range(value.shape[1] // 128):
            tile = value[:, 128 * t : 128 * t + 128]
            low = jnp.sum(jnp.where(left, tile, 0.0), axis=1, keepdims=True)
            high = jnp.sum(jnp.where(left, 0.0, tile), axis=1, keepdims=True)
            parts.append(jnp.where(left, low, high))
        return parts[0] if len(parts) == 1 else jnp.concatenate(parts, axis=1)

    def total(sums):
        return [segments(jnp.sum(part, axis=0, keepdims=True)) for part in sums]

    def build_x():
        near_h = jnp.dot(hot[...], dh[...], preferred_element_type=F32)
        near_l = jnp.dot(hot[...], dl[...], preferred_element_type=F32)
        for hl, (own, near_v) in enumerate(((dh, near_h), (dl, near_l))):
            for p in range(2):
                cols = slice(128 * p, 128 * p + 128)
                nat = [own[0:16, cols].astype(F32)] + [near_v[16 * k : 16 * k + 16, cols] for k in range(8)]
                rot = [pltpu.roll(part, 64, 1) for part in nat]
                for half in range(2):
                    some = slice(8 * half, 8 * half + 8)
                    at = slice((hl * 2 + p) * 16, (hl * 2 + p) * 16 + 16)
                    for m in range(4):
                        a, b = 2 * m, 2 * m + 1
                        low = jnp.where(left8, nat[a][some], rot[b][some])
                        high = jnp.where(left8, rot[a][some], nat[b][some])
                        xp[half, at, 128 * m : 128 * m + 128] = jnp.concatenate([low, high], axis=0).astype(BF16)
                    both = jnp.concatenate([nat[8][some], rot[8][some]], axis=0)
                    xp[half, at, 512:576] = both[:, 0:64].astype(BF16)

    def apply_group(g):
        half = g // 2
        one = jnp.dot(xp[half], wh[g], preferred_element_type=F32)
        two = jnp.dot(xp[half, 0:32, :], wl[g], preferred_element_type=F32)
        both = one[0:32] + one[32:64] + two
        r = lax.broadcasted_iota(I32, (32, 256), 0) & 7
        c = lax.broadcasted_iota(I32, (32, 256), 1) >> 6
        return jnp.where(r == c + 4 * (g % 2), both, 0.0)

    def image(both):
        both = both[:, 0:128] + both[:, 128:256]
        both = both + pltpu.roll(both, 64, 1)
        return jnp.concatenate(
            [jnp.where(left8, both[16 * p : 16 * p + 8], both[16 * p + 8 : 16 * p + 16]) for p in range(2)], axis=1
        )

    def apply_all():
        groups = [apply_group(g) for g in range(4)]
        return [image(groups[0] + groups[1]), image(groups[2] + groups[3])]

    rows_of = [slice(32 * i, 32 * i + 32) for i in range(8)]

    take(0)
    relay(1)
    pltpu.make_async_copy(bb.at[pl.ds(1, 15)], bb.at[pl.ds(1, 15)], b_rx).wait()
    for p in range(2):
        z0[0:16, 128 * p : 128 * p + 128] = bb[:, p, :]
    spread(z0, 0)
    relay(2)
    take(1)
    take(7)
    relay(3)
    take(2)
    take(6)
    arrived(z0, 0)
    sums = jnp.zeros((8, 256), F32)
    for rows in rows_of:
        part = z0[rows, :]
        dh[rows, :], dl[rows, :] = split(part)
        sums = sums + fold8(part * part)
    build_x()
    beta = jnp.sqrt(total([sums])[0])
    s0 = 1.0 / beta
    acc[...] = apply_group(0)
    last_block(0, 4)
    take(3)
    last_block(1, 5)
    z1[0:8, :] = image(acc[...] + apply_group(1)) * s0
    spread(z1, 1, 0, 8)
    last_block(2, 6, 3, 7, 8)
    take(5)
    acc[...] = apply_group(3)
    take(4)

    z1[8:16, :] = image(acc[...] + apply_group(2)) * s0
    spread(z1, 1, 8, 8)
    slots, rest = divmod(sum(sent), 2 * CH)
    got(opb.at[pl.ds(0, slots)], op_tx)
    if rest:
        got(opb.at[0, 0, pl.ds(0, rest)], op_tx)
    arrived(z1, 1)
    sums = jnp.zeros((8, 256), F32)
    for rows in rows_of:
        part = z1[rows, :]
        dh[rows, :], dl[rows, :] = split(part)
        sums = sums + fold8(z0[rows, :] * part)
    build_x()
    h00 = total([sums])[0] * s0
    f0 = h00 * s0
    sums = jnp.zeros((8, 256), F32)
    for rows in rows_of:
        part = z1[rows, :] - f0 * z0[rows, :]
        w1[rows, :] = part
        sums = sums + fold8(part * part)
    h10 = jnp.sqrt(total([sums])[0])
    s1 = 1.0 / h10

    for half, part in enumerate(apply_all()):
        some = slice(8 * half, 8 * half + 8)
        z2[some, :] = (part - h00 * z1[some, :]) * s1
    spread(z2, 2)
    r0 = jnp.sqrt(h00 * h00 + h10 * h10)
    i0 = 1.0 / r0
    c0, n0 = h00 * i0, h10 * i0
    g0, g1 = c0 * beta, -n0 * beta
    arrived(z2, 2)
    sums0, sums1 = jnp.zeros((8, 256), F32), jnp.zeros((8, 256), F32)
    for rows in rows_of:
        part = z2[rows, :]
        dh[rows, :], dl[rows, :] = split(part)
        sums0 = sums0 + fold8(z0[rows, :] * part)
        sums1 = sums1 + fold8(w1[rows, :] * part)
    build_x()
    h01, h11 = total([sums0, sums1])
    h01, h11 = h01 * s0, h11 * s1
    f0, f1 = h01 * s0, h11 * s1
    sums = jnp.zeros((8, 256), F32)
    for rows in rows_of:
        part = z2[rows, :] - f0 * z0[rows, :] - f1 * w1[rows, :]
        if rows.start == 0:
            w2[...] = part[0:16]
        sums = sums + fold8(part * part)
    h21 = jnp.sqrt(total([sums])[0])
    s2 = 1.0 / h21
    last = []
    for half, part in enumerate(apply_all()):
        some = slice(8 * half, 8 * half + 8)
        last.append((part - h01 * z1[some, :] - h11 * z2[some, :]) * s2)
    last = jnp.concatenate(last, axis=0)

    basis = [z0[0:16, :] * s0, w1[0:16, :] * s1, w2[...] * s2]
    sums = [jnp.sum(fold8(part * last), axis=0, keepdims=True) for part in basis + [last]]
    sums = segments(jnp.concatenate([part[:, 128 * p : 128 * p + 128] for part in sums for p in range(2)], axis=0))
    lane8 = lax.broadcasted_iota(I32, (8, 128), 1)
    eighth = (lane8 >> 3 & 7) == lax.broadcasted_iota(I32, (8, 128), 0)
    pd[0] = jnp.sum(jnp.where(eighth, sums, 0.0), axis=0, keepdims=True)
    for dx, dy in peers_p:
        pltpu.make_async_remote_copy(
            src_ref=pd.at[0], dst_ref=pd.at[(-dx) % NX * NY + (-dy) % NY],
            send_sem=z_tx.at[3], recv_sem=z_rx.at[3], device_id=plane(dx, dy), device_id_type=MESH,
        ).start()
    t0, t1 = c0 * h01 + n0 * h11, c0 * h11 - n0 * h01
    r1 = jnp.sqrt(t1 * t1 + h21 * h21)
    i1 = 1.0 / r1
    c1, n1 = t1 * i1, h21 * i1
    g1, g2 = c1 * g1, -n1 * g1
    pltpu.make_async_copy(pd.at[pl.ds(1, 15)], pd.at[pl.ds(1, 15)], z_rx.at[3]).wait()
    dots = jnp.broadcast_to(jnp.sum(pd[...], axis=0), (8, 128))
    dots = segments(jnp.where(eighth & ((lane8 & 7) == 0), dots, 0.0))
    h02, h12, h22, zz = [jnp.concatenate([dots[2 * i : 2 * i + 1], dots[2 * i + 1 : 2 * i + 2]], axis=1) for i in range(4)]
    norm_sq = jnp.maximum(zz - h02 * h02 - h12 * h12 - h22 * h22, 0.0)
    u0, u1 = c0 * h02 + n0 * h12, c0 * h12 - n0 * h02
    u1, u2 = c1 * u1 + n1 * h22, c1 * h22 - n1 * u1
    y2 = u2 * g2 / (u2 * u2 + norm_sq)
    y1 = (g1 - u1 * y2) * i1
    y0 = (g0 - t0 * y1 - u0 * y2) * i0
    result = y0 * basis[0] + y1 * basis[1] + y2 * basis[2]
    for p in range(2):
        sb[:, p, :] = result[:, 128 * p : 128 * p + 128]
    for e, q in peers_z:
        pltpu.make_async_remote_copy(
            src_ref=sb.at[2 * e + q], dst_ref=ob.at[grp], send_sem=s_tx, recv_sem=s_rx,
            device_id={"grp": in_grp(e, q), "sub": sub}, device_id_type=MESH,
        ).start()
    ob[grp] = sb[0]
    pltpu.make_async_copy(pb.at[pl.ds(1, 15)], pb.at[pl.ds(1, 15)], b_tx).wait()
    for n, buf in enumerate((z0, z1, z2)):
        pltpu.make_async_copy(buf.at[pl.ds(16, 240)], buf.at[pl.ds(16, 240)], z_tx.at[n]).wait()
    pltpu.make_async_copy(pd.at[pl.ds(1, 15)], pd.at[pl.ds(1, 15)], z_tx.at[3]).wait()
    pltpu.make_async_copy(sb.at[pl.ds(1, 15)], sb.at[pl.ds(1, 15)], s_tx).wait()
    pltpu.make_async_copy(ob.at[pl.ds(1, 15)], ob.at[pl.ds(1, 15)], s_rx).wait()
    tiles = [ob[:, p, :] for p in range(2)]
    out_ref[0] = jnp.concatenate(
        [tiles[0][:, 0:64], tiles[0][:, 64:128], tiles[1][:, 0:64], tiles[1][:, 64:128]], axis=0
    ).T


def per_device(coarse_op, right_side, owner_map, neighbor_table):
    vmem = pl.BlockSpec(memory_space=pltpu.VMEM)
    dma = pltpu.SemaphoreType.DMA
    return pl.pallas_call(
        kernel,
        out_shape=jax.ShapeDtypeStruct((1, 64, 64), F32),
        in_specs=[pl.BlockSpec(memory_space=pl.ANY)] * 4,
        out_specs=vmem,
        scratch_shapes=[
            pltpu.VMEM((64, 64), F32),
            pltpu.VMEM((1, 256), I32),
            pltpu.VMEM((8, 256), I32),
            pltpu.VMEM((64, 576), F32),
            pltpu.VMEM((NZ, 2, CH, 32, 128), F32),
            pltpu.VMEM((4, 576, 256), BF16),
            pltpu.VMEM((4, 576, 256), BF16),
            pltpu.VMEM((16, 2, 128), F32),
            pltpu.VMEM((16, 2, 128), F32),
            pltpu.VMEM((256, 256), F32),
            pltpu.VMEM((256, 256), F32),
            pltpu.VMEM((256, 256), F32),
            pltpu.VMEM((256, 256), F32),
            pltpu.VMEM((16, 256), F32),
            pltpu.VMEM((256, 256), BF16),
            pltpu.VMEM((256, 256), BF16),
            pltpu.VMEM((128, 256), BF16),
            pltpu.VMEM((2, 64, 576), BF16),
            pltpu.VMEM((32, 256), F32),
            pltpu.VMEM((16, 1, 128), F32),
            pltpu.VMEM((16, 2, 128), F32),
            pltpu.VMEM((16, 2, 128), F32),
            dma((NZ, 5)),
            dma((CH,)),
            dma((NZ,)),
            dma,
            dma((4,)),
            dma,
            dma,
            dma((4,)),
            dma((4,)),
            dma,
            dma,
        ],
        compiler_params=pltpu.CompilerParams(collective_id=0, has_side_effects=True),
    )(coarse_op, right_side, owner_map.reshape(1, 256), neighbor_table.T)


def solution(mesh):
    placed = (P(("grp", "sub"), None, None), P(("grp", "sub"), None, None), P(), P())
    return jax.shard_map(
        per_device,
        mesh=mesh,
        in_specs=placed,
        out_specs=P(("grp", "sub"), None, None),
        check_vma=False,
    )
```
